32 devices in a mesh: img: 2 (over y), row: 8 (over z, x), col: 2 (over core).
Axes of the slice: x: 2, y: 2, z: 4, core: 2. Of those that a mesh axis runs over, the one named last changes fastest.
Arguments:
- features: bfloat16 [16, 128, 512], P(('img', 'row'), 'col'), parts along dimension 0, may hold values from -60 to 60
- first_gain: float32 [512], replicated, may hold values from 0.1 to 1.9
- first_shift: float32 [512], replicated, may hold values from -2.5 to 2.5
- first_weight: bfloat16 [3, 3, 512, 512], P(None, None, 'row'), may hold values from -0.09375 to 0.09375
- first_bias: float32 [512], replicated, may hold values from -2.5 to 2.5
- second_gain: float32 [512], replicated, may hold values from 0.1 to 1.9
- second_shift: float32 [512], replicated, may hold values from -2.5 to 2.5
- second_weight: bfloat16 [3, 3, 512, 512], P(None, None, 'row'), may hold values from -0.09375 to 0.09375
- second_bias: float32 [512], replicated, may hold values from -2.5 to 2.5
- upsample_weight: bfloat16 [3, 3, 512, 512], P(None, None, 'row'), may hold values from -0.09375 to 0.09375
- upsample_bias: float32 [512], replicated, may hold values from -2.5 to 2.5
Outputs:
- upsampled: bfloat16 [32, 256, 512], P(('img', 'row'), 'col'), parts along dimension 0
The draws below stay inside these ranges and needn't reach their ends.
There are 2 independent parts, one for each index of `img`. The reference program is written for one: setup_inputs(seed, part) draws one part's arguments, and reference() takes and returns one part's arrays. A program takes and returns all parts, laid end to end along the dimension named above; an argument that names none is the same for every part. Nothing has to cross between parts.
All inputs are finite; a program needn't handle non-finite values.
Results may differ from the reference program's by a relative error of at most 0.0075.
Values may be sent and summed in bfloat16 or wider, within the bound.
A program may use at most 128 MiB of HBM per device.

```python
import math
import jax
import jax.numpy as jnp
from jax import lax

C = 512
G = 32
H = 8
W = 128


def draw_features(key, part):
    subkeys = jax.random.split(key, 4)
    heights = jnp.arange(H, dtype=jnp.float32) / max(H - 1, 1)
    trend = jnp.exp(heights * math.log(3.0))
    row_jitter = jnp.exp(jax.random.uniform(subkeys[1], (H,), jnp.float32, 0.0, math.log(1.6)))
    column_jitter = jnp.exp(jax.random.uniform(subkeys[2], (W,), jnp.float32, 0.0, math.log(1.6)))
    channel_scale = jnp.exp(jax.random.uniform(subkeys[3], (C,), jnp.float32, math.log(0.7), math.log(1.4)))
    base = jnp.clip(jax.random.normal(subkeys[0], (H, W, C), jnp.float32), -5.0, 5.0)
    scale = trend[:, None, None] * row_jitter[:, None, None] * column_jitter[None, :, None] * channel_scale[None, None, :]
    return (base * scale).astype(jnp.bfloat16)


def level_of(stream_key, shape, shards, smallest, high):
    def one(axis_at, shards_of):
        steps = jax.random.uniform(jax.random.fold_in(jax.random.fold_in(stream_key, 6), axis_at), (shards_of,), jnp.float32, smallest / len(shards), high / len(shards))
        return jnp.repeat(jnp.exp(steps), shape[axis_at] // shards_of).reshape((-1,) + (1,) * (len(shape) - axis_at - 1))

    loudness = one(*shards[0])
    for cut in shards[1:]:
        loudness = loudness * one(*cut)
    return loudness


def bell_draw(rng, extent, spread, reach, shards=(), held_as=jnp.bfloat16):
    values = jax.random.normal(rng, extent, jnp.float32) * spread
    if len(shards) > 0:
        values = level_of(rng, extent, shards, -0.22, 0.18) * values
    return jnp.clip(values, min=-reach, max=reach).astype(held_as)


def setup_inputs(seed: int = 0, part: int = 0) -> dict:
    streams_of = jax.random.split(jax.random.key(seed), 12)
    part_splits = jax.random.split(jax.random.fold_in(streams_of[11], part), 12)
    return {
        "features": draw_features(jax.random.fold_in(jax.random.fold_in(streams_of[11], part), 71), part),
        "first_gain": jnp.clip(1.0 + 0.18 * jax.random.normal(streams_of[1], (C,), jnp.float32), 0.1, 1.9),
        "first_shift": bell_draw(streams_of[2], (C,), 0.5, 2.5, (), jnp.float32),
        "first_weight": bell_draw(streams_of[3], (3, 3, C, C), (9 * C) ** -0.5, 0.09375, ((2, 8),)),
        "first_bias": bell_draw(streams_of[4], (C,), 0.5, 2.5, (), jnp.float32),
        "second_gain": jnp.clip(1.0 + 0.18 * jax.random.normal(streams_of[5], (C,), jnp.float32), 0.1, 1.9),
        "second_shift": bell_draw(streams_of[6], (C,), 0.5, 2.5, (), jnp.float32),
        "second_weight": bell_draw(streams_of[7], (3, 3, C, C), (9 * C) ** -0.5, 0.09375, ((2, 8),)),
        "second_bias": bell_draw(streams_of[8], (C,), 0.5, 2.5, (), jnp.float32),
        "upsample_weight": bell_draw(streams_of[9], (3, 3, C, C), (9 * C) ** -0.5, 0.09375, ((2, 8),)),
        "upsample_bias": bell_draw(streams_of[10], (C,), 0.5, 2.5, (), jnp.float32),
    }


EPS = 1e-06

def group_norm_silu(values, gain, shift):
    height, breadth, channels = values.shape
    grouped = values.reshape(height * breadth, G, channels // G)
    total = lax.optimization_barrier(jnp.sum(grouped, axis=(0, 2)))
    squares = lax.optimization_barrier(jnp.sum(grouped * grouped, axis=(0, 2)))
    count = height * breadth * (channels // G)
    mean = total / count
    var = squares / count - mean * mean
    factor = lax.rsqrt(var + EPS)
    normed = (grouped - mean[None, :, None]) * factor[None, :, None]
    normed = normed.reshape(height, breadth, channels) * gain + shift
    return jax.nn.silu(normed).astype(jnp.bfloat16)

def convolve(inputs, weight, bias):
    result = lax.conv_general_dilated(inputs.astype(jnp.float32)[None], weight.astype(jnp.float32), (1, 1), 'SAME', dimension_numbers=('NHWC', 'HWIO', 'NHWC'), precision=lax.Precision.HIGHEST)
    return result[0] + bias

def reference(features, first_gain, first_shift, first_weight, first_bias, second_gain, second_shift, second_weight, second_bias, upsample_weight, upsample_bias):
    normed_one = group_norm_silu(features.astype(jnp.float32), first_gain, first_shift)
    hidden = convolve(normed_one, first_weight, first_bias).astype(jnp.bfloat16)
    normed_two = group_norm_silu(hidden.astype(jnp.float32), second_gain, second_shift)
    block_out = (convolve(normed_two, second_weight, second_bias) + features.astype(jnp.float32)).astype(jnp.bfloat16)
    doubled = jnp.repeat(jnp.repeat(block_out, 2, axis=0), 2, axis=1)
    return convolve(doubled, upsample_weight, upsample_bias).astype(jnp.bfloat16)
```

```python
import jax
import jax.numpy as jnp
from jax import lax
from jax.experimental import pallas as pl
from jax.experimental.pallas import tpu as pltpu
from jax.sharding import PartitionSpec as P

G = 32


EPS = 1e-06


def extended(cells, sides, width):
    for axis, dim in sides:
        count = lax.axis_size(axis)
        ends = count - 1
        head = lax.slice_in_dim(cells, 0, width, axis=dim)
        tail = lax.slice_in_dim(cells, cells.shape[dim] - width, cells.shape[dim], axis=dim)
        cells = jnp.concatenate(
            [
                lax.ppermute(tail, axis, [(i, (i + 1) % count) for i in range(ends)]),
                cells,
                lax.ppermute(head, axis, [((i + 1) % count, i) for i in range(ends)]),
            ],
            axis=dim,
        )
    return cells


def norm_silu(values, gain, shift):
    height, breadth, channels = values.shape
    grouped = values.reshape(height * breadth, G, channels // G)
    total = jnp.sum(grouped, axis=(0, 2))
    squares = jnp.sum(grouped * grouped, axis=(0, 2))
    total, squares = lax.psum((total, squares), ("row", "col"))
    count = height * breadth * lax.axis_size("row") * lax.axis_size("col") * (channels // G)
    mean = total / count
    var = squares / count - mean * mean
    factor = lax.rsqrt(var + EPS)
    normed = (grouped - mean[None, :, None]) * factor[None, :, None]
    normed = normed.reshape(height, breadth, channels) * gain + shift
    return jax.nn.silu(normed).astype(jnp.bfloat16)


def extend(values):
    return extended(values, (("row", 0), ("col", 1)), 1)


def convolve(padded, weight, bias, height, breadth):
    outputs = weight.shape[3]
    empty = jnp.zeros((height, breadth, outputs), jnp.float32)
    share = weight.shape[2] // lax.axis_size("col")
    own = lax.dynamic_slice_in_dim(weight, lax.axis_index("col") * share, share, 2)
    total = empty
    piece = lax.all_gather(own, ("row", "col"), axis=2, tiled=True)
    depth = piece.shape[2]
    offset = jnp.asarray(jnp.int32(0), jnp.int32)
    for offset_y in range(3):
        for offset_x in range(3):
            window = lax.dynamic_slice(
                padded, (jnp.int32(offset_y), jnp.int32(offset_x), offset), (height, breadth, depth)
            )
            total = total + jnp.einsum(
                "hwk,kc->hwc", window, piece[offset_y, offset_x], preferred_element_type=jnp.float32
            )
    return total + bias


def on_device(
    features,
    first_gain,
    first_shift,
    first_weight,
    first_bias,
    second_gain,
    second_shift,
    second_weight,
    second_bias,
    upsample_weight,
    upsample_bias,
):
    height, breadth, channels = features.shape
    normed_one = norm_silu(features.astype(jnp.float32), first_gain, first_shift)
    hidden = convolve(extend(normed_one), first_weight, first_bias, height, breadth).astype(
        jnp.bfloat16
    )
    normed_two = norm_silu(hidden.astype(jnp.float32), second_gain, second_shift)
    block_out = (
        convolve(extend(normed_two), second_weight, second_bias, height, breadth)
        + features.astype(jnp.float32)
    ).astype(jnp.bfloat16)
    doubled = jnp.repeat(jnp.repeat(block_out, 2, axis=0), 2, axis=1)
    padded = extend(doubled)
    return convolve(padded, upsample_weight, upsample_bias, 2 * height, 2 * breadth).astype(
        jnp.bfloat16
    )


def fused_kernel(
    features,
    gain_one,
    shift_one,
    bias_one,
    gain_two,
    shift_two,
    bias_two,
    bias_up,
    weight_one,
    weight_two,
    weight_up,
    out,
    fbuf,
    xs,
    taps,
    gathered,
    parts,
    sums,
    hbuf,
    stats,
    own_block,
    b3,
    x3,
    mixed,
    swap,
    local_sem,
    wx_send,
    wx_recv,
    f_send,
    f_recv,
    rs_send,
    rs_recv,
    h_send,
    h_recv,
    b_send,
    b_recv,
    ring_send,
    ring_recv,
    y_send,
    y_recv,
    o_send,
    o_recv,
):
    img = lax.axis_index("img")
    row = lax.axis_index("row")
    col = lax.axis_index("col")
    rows = lax.axis_size("row")
    cuts = rows // 2
    z, x = row // 2, row % 2
    other = 1 - col
    pair = row + 1 - 2 * x
    half_width, channels = features.shape
    width = 2 * half_width
    block = channels // cuts
    share = channels // rows
    outs = channels // 2
    near = rows // 2
    f32, bf16 = jnp.float32, jnp.bfloat16
    pending = []

    def remote(src, dst, send, recv, **device):
        return pltpu.make_async_remote_copy(
            src_ref=src,
            dst_ref=dst,
            send_sem=send,
            recv_sem=recv,
            device_id=device,
            device_id_type=pl.DeviceIdType.MESH,
        )

    zero_rows = jnp.zeros((2, width, block), bf16)
    for parity in range(2):
        for slot in (0, 2):
            b3[parity, slot] = zero_rows

    barrier = pltpu.get_barrier_semaphore()
    for step in range(rows):
        for side in range(2):
            if step or side:
                pl.semaphore_signal(
                    barrier,
                    inc=1,
                    device_id={"row": (row + step) % rows, "col": (col + side) % 2},
                    device_id_type=pl.DeviceIdType.MESH,
                )
    pl.semaphore_signal(
        barrier, inc=1, device_id={"img": 1 - img}, device_id_type=pl.DeviceIdType.MESH
    )
    pl.semaphore_wait(barrier, 2 * rows)

    lanes = pl.ds(pl.multiple_of(col * outs, outs), outs)
    mine = pl.ds(pl.multiple_of(x * share, share), share)

    def feature_copy(step):
        target = (row + step) % rows
        part = pl.ds(pl.multiple_of((target // 2) * block, block), block)
        return remote(
            features.at[:, part], fbuf.at[col, row], f_send.at[step], f_recv.at[row], row=target
        )

    for step in range(1, rows):
        copy = feature_copy(step)
        copy.start()
        pending.append(copy)
    fbuf[col, row] = features[:, pl.ds(pl.multiple_of(z * block, block), block)]

    local = []
    for index, weight in enumerate((weight_one, weight_two)):
        copy = remote(
            weight.at[:, :, :, lanes],
            taps.at[index, :, :, mine, :],
            wx_send.at[index],
            wx_recv.at[index],
            row=pair,
        )
        copy.start()
        pending.append(copy)
        copy = pltpu.make_async_copy(
            weight.at[:, :, :, lanes], taps.at[index, :, :, mine, :], local_sem.at[index]
        )
        copy.start()
        local.append(copy)
    copy = pltpu.make_async_copy(
        weight_up.at[:, :, :, lanes],
        gathered.at[:, :, pl.ds(pl.multiple_of(row * share, share), share), :],
        local_sem.at[2],
    )
    copy.start()
    local.append(copy)

    place = z * (1 - x) + (rows - 1 - z) * x
    piece = share // 2

    def row_at(position):
        side = position // near
        return (1 - side) * 2 * position + side * (2 * (rows - 1 - position) + 1)

    after = row_at((place + 1) % rows)
    before = row_at((place + rows - 1) % rows)

    def unit(position, part):
        return gathered.at[
            :, :, pl.ds(pl.multiple_of(row_at(position) * share + part * piece, piece), piece), :
        ]

    def ring_copy(way, step):
        position = (place + rows - (step - 1)) % rows if way == 0 else (place + step - 1) % rows
        if step == 1:
            src = weight_up.at[:, :, pl.ds(pl.multiple_of(img * piece, piece), piece), lanes]
        else:
            src = unit(position, img)
        return remote(
            src,
            unit(position, img),
            ring_send.at[way, step - 1],
            ring_recv.at[way, step - 1],
            row=after if way == 0 else before,
        )

    reach = (near, rows - 1 - near)

    def cross_copy(way, step, half):
        position = (place + rows - step) % rows if way == 0 else (place + step) % rows
        return remote(
            unit(position, half),
            unit(position, half),
            y_send.at[way, step - 1],
            y_recv.at[way, step - 1],
            img=1 - img,
        )

    def start_ring(step):
        for way in range(2):
            if step <= reach[way]:
                copy = ring_copy(way, step)
                copy.start()
                pending.append(copy)

    def arrived_ring(way, step):
        position = (place + rows - step) % rows if way == 0 else (place + step) % rows
        return remote(
            unit(position, img),
            unit(position, img),
            ring_send.at[way, step - 1],
            ring_recv.at[way, step - 1],
            row=after,
        )

    def turn_ring(step):
        for way in range(2):
            if step <= reach[way]:
                arrived_ring(way, step).wait_recv()
        start_ring(step + 1)
        for way in range(2):
            if step <= reach[way]:
                copy = cross_copy(way, step, img)
                copy.start()
                pending.append(copy)

    start_ring(1)

    for step in range(1, rows):
        origin = (row + step) % rows
        remote(
            features.at[:, pl.ds(0, block)],
            fbuf.at[col, origin],
            f_send.at[step],
            f_recv.at[origin],
            row=pair,
        ).wait_recv()
    copy = remote(fbuf.at[col], fbuf.at[col], f_send.at[0], f_recv.at[rows], col=other)
    copy.start()
    pending.append(copy)
    remote(fbuf.at[other], fbuf.at[other], f_send.at[0], f_recv.at[rows], col=other).wait_recv()

    same = (
        lax.broadcasted_iota(jnp.int32, (block, block), 0) // (channels // G)
        == lax.broadcasted_iota(jnp.int32, (block, block), 1) // (channels // G)
    ).astype(f32)
    count = rows * width * (channels // G)

    def moments(total, squares):
        both = jnp.concatenate([total, squares, jnp.zeros((6, block), f32)], axis=0)
        both = jnp.dot(both, same, precision=lax.Precision.HIGHEST, preferred_element_type=f32)
        mean = both[0:1] / count
        var = both[1:2] / count - mean * mean
        return mean, lax.rsqrt(var + EPS)

    here = pl.ds(pl.multiple_of(z * block, block), block)
    first_column = lax.broadcasted_iota(jnp.int32, (width, block), 0) == 0
    last_column = lax.broadcasted_iota(jnp.int32, (width, block), 0) == width - 1

    def fill(slot, values, mean, factor, gain, shift):
        normed = (values - mean) * factor * gain + shift
        normed = normed / (1.0 + jnp.exp(-normed))
        if slot == 0:
            normed = jnp.where(x == 0, 0.0, normed)
        if slot == near + 1:
            normed = jnp.where(x == 1, 0.0, normed)
        left = jnp.where(first_column, 0.0, pltpu.roll(normed, 1, 0))
        right = jnp.where(last_column, 0.0, pltpu.roll(normed, width - 1, 0))
        xs[slot, :, 0:block] = left.astype(bf16)
        xs[slot, :, block : 2 * block] = normed.astype(bf16)
        xs[slot, :, 2 * block : 3 * block] = right.astype(bf16)

    def feature_row(index):
        return jnp.concatenate([fbuf[0, index], fbuf[1, index]], axis=0).astype(f32)

    total = jnp.zeros((1, block), f32)
    squares = jnp.zeros((1, block), f32)
    for index in range(rows):
        values = feature_row(index)
        total += jnp.sum(values, axis=0, keepdims=True)
        squares += jnp.sum(values * values, axis=0, keepdims=True)
    mean, factor = moments(total, squares)
    for slot in range(near + 2):
        index = jnp.clip(near * x - 1 + slot, 0, rows - 1)
        fill(slot, feature_row(index), mean, factor, gain_one[:, here], shift_one[:, here])

    tile = near * width // 2

    def partial_conv(index):
        local[index].wait()
        remote(
            weight_one.at[:, :, :, lanes],
            taps.at[index, :, :, pl.ds(pl.multiple_of((1 - x) * share, share), share), :],
            wx_send.at[index],
            wx_recv.at[index],
            row=pair,
        ).wait_recv()
        for side in range(2):
            acc = jnp.zeros((tile, outs), f32)
            for a in range(3):
                first = a + side * near // 2
                acc += jnp.dot(
                    xs[first : first + near // 2].reshape(tile, 3 * block),
                    taps[index, a].reshape(3 * block, outs),
                    preferred_element_type=f32,
                )
            for j in range(2):
                parts[index, j, side] = acc[:, j * block : (j + 1) * block].astype(bf16)
                target = 2 * col + j
                itself = jnp.logical_and(target == z, col == side)
                copy = remote(
                    parts.at[index, j, side],
                    sums.at[index, z],
                    rs_send.at[index, j, side],
                    rs_recv.at[index, z],
                    row=2 * target + x,
                    col=side,
                )

                @pl.when(itself)
                def _():
                    sums[index, z] = parts[index, j, side]

                @pl.when(jnp.logical_not(itself))
                def _():
                    copy.start()

    def partial_sent(index):
        for side in range(2):
            for j in range(2):
                target = 2 * col + j

                @pl.when(jnp.logical_not(jnp.logical_and(target == z, col == side)))
                def _():
                    remote(
                        parts.at[index, j, side],
                        sums.at[index, z],
                        rs_send.at[index, j, side],
                        rs_recv.at[index, z],
                        row=2 * target + x,
                        col=side,
                    ).wait_send()

    def reduced(index, bias):
        for origin in range(cuts):

            @pl.when(jnp.logical_not(jnp.logical_and(z == origin, z // 2 == col)))
            def _():
                remote(
                    parts.at[index, 0, 0],
                    sums.at[index, origin],
                    rs_send.at[index, 0, 0],
                    rs_recv.at[index, origin],
                    row=pair,
                ).wait_recv()

        result = sums[index, 0].astype(f32)
        for origin in range(1, cuts):
            result += sums[index, origin].astype(f32)
        return result + bias[:, here]

    partial_conv(0)
    turn_ring(1)

    hidden = reduced(0, bias_one).astype(bf16)
    start = 1 + 2 * col
    hbuf[pl.ds(start, 2)] = hidden.reshape(2, width, block)
    hidden = hidden.astype(f32)
    group = 2 * x + col
    stats[group] = jnp.concatenate(
        [
            jnp.sum(hidden, axis=0, keepdims=True),
            jnp.sum(hidden * hidden, axis=0, keepdims=True),
            jnp.zeros((6, block), f32),
        ],
        axis=0,
    )
    for step, (target_row, target_col) in enumerate(((row, other), (pair, col), (pair, other))):
        copy = remote(
            stats.at[group],
            stats.at[group],
            h_send.at[step],
            h_recv.at[group],
            row=target_row,
            col=target_col,
        )
        copy.start()
        pending.append(copy)
    copy = remote(
        hbuf.at[pl.ds(start, 2)], hbuf.at[pl.ds(start, 2)], h_send.at[3], h_recv.at[4], col=other
    )
    copy.start()
    pending.append(copy)

    def edge(side):
        return remote(
            hbuf.at[near - (near - 1) * x],
            hbuf.at[(near + 1) * x],
            h_send.at[4 + side],
            h_recv.at[5],
            row=pair,
            col=side,
        )

    @pl.when(col == 1 - x)
    def _():
        for side in range(2):
            edge(side).start()

    turn_ring(2)
    for who in range(4):

        @pl.when(group != who)
        def _():
            remote(
                stats.at[who], stats.at[who], h_send.at[0], h_recv.at[who], row=pair
            ).wait_recv()

    theirs = hbuf.at[pl.ds(1 + 2 * other, 2)]
    remote(theirs, theirs, h_send.at[3], h_recv.at[4], col=other).wait_recv()
    remote(
        hbuf.at[0], hbuf.at[(near + 1) * (1 - x)], h_send.at[4], h_recv.at[5], row=pair
    ).wait_recv()
    both = stats[0] + stats[1] + stats[2] + stats[3]
    mean, factor = moments(both[0:1], both[1:2])
    for slot in range(near + 2):
        values = hbuf[slot].astype(f32)
        if slot == 0:
            values = jnp.where(x == 0, 0.0, values)
        if slot == near + 1:
            values = jnp.where(x == 1, 0.0, values)
        fill(slot, values, mean, factor, gain_two[:, here], shift_two[:, here])

    partial_conv(1)
    turn_ring(3)

    residual = jnp.concatenate(
        [feature_row(near * x + 2 * col), feature_row(near * x + 2 * col + 1)], axis=0
    )
    own_block[...] = (reduced(1, bias_two) + residual).astype(bf16).reshape(2, width, block)

    def block_copies(act):
        for k in range(2):
            origin = near * x + 2 * col + k
            for d in (-1, 0, 1):
                target = origin + d
                valid = jnp.logical_and(target >= 0, target < rows)
                itself = jnp.logical_and(target == row, z % 2 == col)
                act(k, d, target, valid, itself)

    def block_copy(k, d, target):
        return remote(
            own_block.at[k],
            b3.at[z % 2, 1 - d, z // 2],
            b_send.at[k, d + 1],
            b_recv.at[1 - d, z // 2],
            row=target,
            col=z % 2,
        )

    def begin(k, d, target, valid, itself):
        @pl.when(jnp.logical_and(valid, jnp.logical_not(itself)))
        def _():
            block_copy(k, d, target).start()

        @pl.when(itself)
        def _():
            b3[z % 2, 1 - d, z // 2] = own_block[k]

    def finish(k, d, target, valid, itself):
        @pl.when(jnp.logical_and(valid, jnp.logical_not(itself)))
        def _():
            block_copy(k, d, target).wait_send()

    block_copies(begin)
    turn_ring(4)
    for slot in range(3):
        source = row + slot - 1
        valid = jnp.logical_and(source >= 0, source < rows)
        for half in range(2):
            block_of = 2 * half + col
            itself = jnp.logical_and(
                jnp.logical_and(block_of == z, source // near == x), (source // 2) % 2 == col
            )

            @pl.when(jnp.logical_and(valid, jnp.logical_not(itself)))
            def _():
                remote(
                    own_block.at[0],
                    b3.at[col, slot, half],
                    b_send.at[0, 0],
                    b_recv.at[slot, half],
                    row=pair,
                ).wait_recv()

    copy = remote(b3.at[col], b3.at[col], b_send.at[2, 0], b_recv.at[3, 0], col=other)
    copy.start()
    pending.append(copy)
    remote(b3.at[other], b3.at[other], b_send.at[2, 0], b_recv.at[3, 0], col=other).wait_recv()

    for slot in range(3):
        for which in range(cuts):
            at = slice(which * block, (which + 1) * block)
            values = b3[which % 2, slot, which // 2]
            wide = values.astype(f32)
            x3[slot, 0, :, at] = jnp.where(first_column, 0.0, pltpu.roll(wide, 1, 0)).astype(bf16)
            x3[slot, 1, :, at] = values
            x3[slot, 2, :, at] = jnp.where(
                last_column, 0.0, pltpu.roll(wide, width - 1, 0)
            ).astype(bf16)

    local[2].wait()
    for way in range(2):
        for step in range(1, reach[way] + 1):
            cross_copy(way, step, 1 - img).wait_recv()

    acc = jnp.zeros((4 * width, outs), f32)
    for a in range(3):
        for c in range(3):
            window = jnp.concatenate(
                [
                    x3[(p + a - 1) // 2 + 1, (q + c - 1) // 2 + 1]
                    for p in range(2)
                    for q in range(2)
                ],
                axis=0,
            )
            acc += jnp.dot(window, gathered[a, c], preferred_element_type=f32)
    acc += bias_up[:, lanes]
    for p in range(2):
        for q in range(2):
            first = (2 * p + q) * width
            for lane in range(outs // 128):
                mixed[lane, p, pl.ds(q, width, stride=2), :] = acc[
                    first : first + width, lane * 128 : (lane + 1) * 128
                ]
    for p in range(2):
        for lane in range(outs // 128):
            at = slice(lane * 128, (lane + 1) * 128)
            swap[p, :, at] = mixed[
                lane, p, pl.ds(pl.multiple_of(other * width, width), width), :
            ].astype(bf16)
    copy = remote(swap, out.at[:, :, lanes], o_send.at[0], o_recv.at[0], col=other)
    copy.start()
    pending.append(copy)
    for p in range(2):
        for lane in range(outs // 128):
            at = pl.ds(pl.multiple_of(col * outs + lane * 128, 128), 128)
            out[p, :, at] = mixed[
                lane, p, pl.ds(pl.multiple_of(col * width, width), width), :
            ].astype(bf16)
    their_lanes = pl.ds(pl.multiple_of(other * outs, outs), outs)
    remote(swap, out.at[:, :, their_lanes], o_send.at[0], o_recv.at[0], col=other).wait_recv()

    for copy in pending:
        copy.wait_send()
    partial_sent(0)
    partial_sent(1)
    block_copies(finish)

    @pl.when(col == 1 - x)
    def _():
        for side in range(2):
            edge(side).wait_send()


def fused(
    features,
    first_gain,
    first_shift,
    first_weight,
    first_bias,
    second_gain,
    second_shift,
    second_weight,
    second_bias,
    upsample_weight,
    upsample_bias,
):
    _, half_width, channels = features.shape
    rows = lax.axis_size("row")
    cuts, near, width = rows // 2, rows // 2, 2 * half_width
    block, outs = channels // cuts, channels // 2
    bf16, f32 = jnp.bfloat16, jnp.float32
    dma = pltpu.SemaphoreType.DMA
    vmem = pl.BlockSpec(memory_space=pltpu.VMEM)
    anywhere = pl.BlockSpec(memory_space=pl.ANY)
    vectors = [
        v.reshape(1, channels)
        for v in (
            first_gain,
            first_shift,
            first_bias,
            second_gain,
            second_shift,
            second_bias,
            upsample_bias,
        )
    ]
    return pl.pallas_call(
        fused_kernel,
        out_shape=jax.ShapeDtypeStruct((2, width, channels), bf16),
        in_specs=[vmem] * 8 + [anywhere] * 3,
        out_specs=vmem,
        scratch_shapes=[
            pltpu.VMEM((2, rows, half_width, block), bf16),
            pltpu.VMEM((near + 2, width, 3 * block), bf16),
            pltpu.VMEM((2, 3, 3, block, outs), bf16),
            pltpu.VMEM((3, 3, channels, outs), bf16),
            pltpu.VMEM((2, 2, 2, near * width // 2, block), bf16),
            pltpu.VMEM((2, cuts, near * width // 2, block), bf16),
            pltpu.VMEM((near + 2, width, block), bf16),
            pltpu.VMEM((4, 8, block), f32),
            pltpu.VMEM((2, width, block), bf16),
            pltpu.VMEM((2, 3, 2, width, block), bf16),
            pltpu.VMEM((3, 3, width, channels), bf16),
            pltpu.VMEM((outs // 128, 2, 2 * width, 128), f32),
            pltpu.VMEM((2, width, outs), bf16),
            dma((3,)),
            dma((2,)),
            dma((2,)),
            dma((rows,)),
            dma((rows + 1,)),
            dma((2, 2, 2)),
            dma((2, cuts)),
            dma((6,)),
            dma((6,)),
            dma((3, 3)),
            dma((4, 2)),
            dma((2, near)),
            dma((2, near)),
            dma((2, near)),
            dma((2, near)),
            dma((1,)),
            dma((1,)),
        ],
        compiler_params=pltpu.CompilerParams(collective_id=0, has_side_effects=True),
    )(features.reshape(half_width, channels), *vectors, first_weight, second_weight, upsample_weight)


def program(features, *others):
    height, half_width, channels = features.shape
    rows = lax.axis_size("row")
    fits = (
        (lax.axis_size("img"), rows, lax.axis_size("col")) == (2, 8, 2)
        and height == 1
        and half_width % 16 == 0
        and channels == rows // 2 * 128
        and 128 % (channels // G) == 0
    )
    return (fused if fits else on_device)(features, *others)


def solution(mesh):
    return jax.shard_map(
        program,
        mesh=mesh,
        in_specs=(
            P(("img", "row"), "col", None),
            P(),
            P(),
            P(None, None, "row", None),
            P(),
            P(),
            P(),
            P(None, None, "row", None),
            P(),
            P(None, None, "row", None),
            P(),
        ),
        out_specs=P(("img", "row"), "col", None),
        check_vma=False,
    )
```

```python
import jax
import jax.numpy as jnp
from jax import lax
from jax.experimental import pallas as pl
from jax.experimental.pallas import tpu as pltpu
from jax.sharding import PartitionSpec as P

G = 32


EPS = 1e-06


def extended(cells, sides, width):
    for axis, dim in sides:
        count = lax.axis_size(axis)
        ends = count - 1
        head = lax.slice_in_dim(cells, 0, width, axis=dim)
        tail = lax.slice_in_dim(cells, cells.shape[dim] - width, cells.shape[dim], axis=dim)
        cells = jnp.concatenate(
            [
                lax.ppermute(tail, axis, [(i, (i + 1) % count) for i in range(ends)]),
                cells,
                lax.ppermute(head, axis, [((i + 1) % count, i) for i in range(ends)]),
            ],
            axis=dim,
        )
    return cells


def norm_silu(values, gain, shift):
    height, breadth, channels = values.shape
    grouped = values.reshape(height * breadth, G, channels // G)
    total = jnp.sum(grouped, axis=(0, 2))
    squares = jnp.sum(grouped * grouped, axis=(0, 2))
    total, squares = lax.psum((total, squares), ("row", "col"))
    count = height * breadth * lax.axis_size("row") * lax.axis_size("col") * (channels // G)
    mean = total / count
    var = squares / count - mean * mean
    factor = lax.rsqrt(var + EPS)
    normed = (grouped - mean[None, :, None]) * factor[None, :, None]
    normed = normed.reshape(height, breadth, channels) * gain + shift
    return jax.nn.silu(normed).astype(jnp.bfloat16)


def extend(values):
    return extended(values, (("row", 0), ("col", 1)), 1)


def convolve(padded, weight, bias, height, breadth):
    outputs = weight.shape[3]
    empty = jnp.zeros((height, breadth, outputs), jnp.float32)
    share = weight.shape[2] // lax.axis_size("col")
    own = lax.dynamic_slice_in_dim(weight, lax.axis_index("col") * share, share, 2)
    total = empty
    piece = lax.all_gather(own, ("row", "col"), axis=2, tiled=True)
    depth = piece.shape[2]
    offset = jnp.asarray(jnp.int32(0), jnp.int32)
    for offset_y in range(3):
        for offset_x in range(3):
            window = lax.dynamic_slice(
                padded, (jnp.int32(offset_y), jnp.int32(offset_x), offset), (height, breadth, depth)
            )
            total = total + jnp.einsum(
                "hwk,kc->hwc", window, piece[offset_y, offset_x], preferred_element_type=jnp.float32
            )
    return total + bias


def on_device(
    features,
    first_gain,
    first_shift,
    first_weight,
    first_bias,
    second_gain,
    second_shift,
    second_weight,
    second_bias,
    upsample_weight,
    upsample_bias,
):
    height, breadth, channels = features.shape
    normed_one = norm_silu(features.astype(jnp.float32), first_gain, first_shift)
    hidden = convolve(extend(normed_one), first_weight, first_bias, height, breadth).astype(
        jnp.bfloat16
    )
    normed_two = norm_silu(hidden.astype(jnp.float32), second_gain, second_shift)
    block_out = (
        convolve(extend(normed_two), second_weight, second_bias, height, breadth)
        + features.astype(jnp.float32)
    ).astype(jnp.bfloat16)
    doubled = jnp.repeat(jnp.repeat(block_out, 2, axis=0), 2, axis=1)
    padded = extend(doubled)
    return convolve(padded, upsample_weight, upsample_bias, 2 * height, 2 * breadth).astype(
        jnp.bfloat16
    )


def fused_kernel(
    features,
    gain_one,
    shift_one,
    bias_one,
    gain_two,
    shift_two,
    bias_two,
    bias_up,
    weight_one,
    weight_two,
    weight_up,
    out,
    fbuf,
    xs,
    taps,
    gathered,
    parts,
    sums,
    hbuf,
    stats,
    own_block,
    b3,
    x3,
    mixed,
    swap,
    local_sem,
    wx_send,
    wx_recv,
    f_send,
    f_recv,
    rs_send,
    rs_recv,
    h_send,
    h_recv,
    b_send,
    b_recv,
    ring_send,
    ring_recv,
    y_send,
    y_recv,
    o_send,
    o_recv,
):
    img = lax.axis_index("img")
    row = lax.axis_index("row")
    col = lax.axis_index("col")
    rows = lax.axis_size("row")
    cuts = rows // 2
    z, x = row // 2, row % 2
    other = 1 - col
    pair = row + 1 - 2 * x
    half_width, channels = features.shape
    width = 2 * half_width
    block = channels // cuts
    share = channels // rows
    outs = channels // 2
    near = rows // 2
    f32, bf16 = jnp.float32, jnp.bfloat16
    pending = []

    def remote(src, dst, send, recv, **device):
        return pltpu.make_async_remote_copy(
            src_ref=src,
            dst_ref=dst,
            send_sem=send,
            recv_sem=recv,
            device_id=device,
            device_id_type=pl.DeviceIdType.MESH,
        )

    zero_rows = jnp.zeros((2, width, block), bf16)
    for parity in range(2):
        for slot in (0, 2):
            b3[parity, slot] = zero_rows

    barrier = pltpu.get_barrier_semaphore()
    for step in range(rows):
        for side in range(2):
            if step or side:
                pl.semaphore_signal(
                    barrier,
                    inc=1,
                    device_id={"row": (row + step) % rows, "col": (col + side) % 2},
                    device_id_type=pl.DeviceIdType.MESH,
                )
    pl.semaphore_signal(
        barrier, inc=1, device_id={"img": 1 - img}, device_id_type=pl.DeviceIdType.MESH
    )
    pl.semaphore_wait(barrier, 2 * rows)

    lanes = pl.ds(pl.multiple_of(col * outs, outs), outs)
    mine = pl.ds(pl.multiple_of(x * share, share), share)

    def feature_copy(step):
        target = (row + step) % rows
        part = pl.ds(pl.multiple_of((target // 2) * block, block), block)
        return remote(
            features.at[:, part], fbuf.at[col, row], f_send.at[step], f_recv.at[row], row=target
        )

    for step in range(1, rows):
        copy = feature_copy(step)
        copy.start()
        pending.append(copy)
    fbuf[col, row] = features[:, pl.ds(pl.multiple_of(z * block, block), block)]

    def start_taps(index):
        copy = remote(
            (weight_one, weight_two)[index].at[:, :, :, lanes],
            taps.at[index, :, :, mine, :],
            wx_send.at[index],
            wx_recv.at[index],
            row=pair,
        )
        copy.start()
        pending.append(copy)

    local = []
    for index, weight in enumerate((weight_one, weight_two)):
        if index == 0:
            start_taps(0)
        copy = pltpu.make_async_copy(
            weight.at[:, :, :, lanes], taps.at[index, :, :, mine, :], local_sem.at[index]
        )
        copy.start()
        local.append(copy)
    copy = pltpu.make_async_copy(
        weight_up.at[:, :, :, lanes],
        gathered.at[:, :, pl.ds(pl.multiple_of(row * share, share), share), :],
        local_sem.at[2],
    )
    copy.start()
    local.append(copy)

    place = z * (1 - x) + (rows - 1 - z) * x
    piece = share // 2

    def row_at(position):
        side = position // near
        return (1 - side) * 2 * position + side * (2 * (rows - 1 - position) + 1)

    after = row_at((place + 1) % rows)
    before = row_at((place + rows - 1) % rows)

    def unit(position, part):
        return gathered.at[
            :, :, pl.ds(pl.multiple_of(row_at(position) * share + part * piece, piece), piece), :
        ]

    def ring_copy(way, step):
        position = (place + rows - (step - 1)) % rows if way == 0 else (place + step - 1) % rows
        if step == 1:
            src = weight_up.at[:, :, pl.ds(pl.multiple_of(img * piece, piece), piece), lanes]
        else:
            src = unit(position, img)
        return remote(
            src,
            unit(position, img),
            ring_send.at[way, step - 1],
            ring_recv.at[way, step - 1],
            row=after if way == 0 else before,
        )

    reach = (near, rows - 1 - near)

    def cross_copy(way, step, half):
        position = (place + rows - step) % rows if way == 0 else (place + step) % rows
        return remote(
            unit(position, half),
            unit(position, half),
            y_send.at[way, step - 1],
            y_recv.at[way, step - 1],
            img=1 - img,
        )

    def start_ring(step):
        for way in range(2):
            if step <= reach[way]:
                copy = ring_copy(way, step)
                copy.start()
                pending.append(copy)

    def arrived_ring(way, step):
        position = (place + rows - step) % rows if way == 0 else (place + step) % rows
        return remote(
            unit(position, img),
            unit(position, img),
            ring_send.at[way, step - 1],
            ring_recv.at[way, step - 1],
            row=after,
        )

    def turn_ring(step):
        for way in range(2):
            if step <= reach[way]:
                arrived_ring(way, step).wait_recv()
        start_ring(step + 1)
        for way in range(2):
            if step <= reach[way]:
                copy = cross_copy(way, step, img)
                copy.start()
                pending.append(copy)

    start_ring(1)

    for step in range(1, rows):
        origin = (row + step) % rows
        remote(
            features.at[:, pl.ds(0, block)],
            fbuf.at[col, origin],
            f_send.at[step],
            f_recv.at[origin],
            row=pair,
        ).wait_recv()
    copy = remote(fbuf.at[col], fbuf.at[col], f_send.at[0], f_recv.at[rows], col=other)
    copy.start()
    pending.append(copy)
    remote(fbuf.at[other], fbuf.at[other], f_send.at[0], f_recv.at[rows], col=other).wait_recv()

    same = (
        lax.broadcasted_iota(jnp.int32, (block, block), 0) // (channels // G)
        == lax.broadcasted_iota(jnp.int32, (block, block), 1) // (channels // G)
    ).astype(f32)
    count = rows * width * (channels // G)

    def moments(total, squares):
        both = jnp.concatenate([total, squares, jnp.zeros((6, block), f32)], axis=0)
        both = jnp.dot(both, same, precision=lax.Precision.HIGHEST, preferred_element_type=f32)
        mean = both[0:1] / count
        var = both[1:2] / count - mean * mean
        return mean, lax.rsqrt(var + EPS)

    here = pl.ds(pl.multiple_of(z * block, block), block)
    first_column = lax.broadcasted_iota(jnp.int32, (width, block), 0) == 0
    last_column = lax.broadcasted_iota(jnp.int32, (width, block), 0) == width - 1

    def fill(slot, values, mean, factor, gain, shift):
        normed = (values - mean) * factor * gain + shift
        normed = normed / (1.0 + jnp.exp(-normed))
        if slot == 0:
            normed = jnp.where(x == 0, 0.0, normed)
        if slot == near + 1:
            normed = jnp.where(x == 1, 0.0, normed)
        left = jnp.where(first_column, 0.0, pltpu.roll(normed, 1, 0))
        right = jnp.where(last_column, 0.0, pltpu.roll(normed, width - 1, 0))
        xs[slot, :, 0:block] = left.astype(bf16)
        xs[slot, :, block : 2 * block] = normed.astype(bf16)
        xs[slot, :, 2 * block : 3 * block] = right.astype(bf16)

    def feature_row(index):
        return jnp.concatenate([fbuf[0, index], fbuf[1, index]], axis=0).astype(f32)

    total = jnp.zeros((1, block), f32)
    squares = jnp.zeros((1, block), f32)
    for index in range(rows):
        values = feature_row(index)
        total += jnp.sum(values, axis=0, keepdims=True)
        squares += jnp.sum(values * values, axis=0, keepdims=True)
    mean, factor = moments(total, squares)
    for slot in range(near + 2):
        index = jnp.clip(near * x - 1 + slot, 0, rows - 1)
        fill(slot, feature_row(index), mean, factor, gain_one[:, here], shift_one[:, here])

    tile = near * width // 2

    def partial_conv(index):
        local[index].wait()
        remote(
            weight_one.at[:, :, :, lanes],
            taps.at[index, :, :, pl.ds(pl.multiple_of((1 - x) * share, share), share), :],
            wx_send.at[index],
            wx_recv.at[index],
            row=pair,
        ).wait_recv()
        for side in range(2):
            acc = jnp.zeros((tile, outs), f32)
            for a in range(3):
                first = a + side * near // 2
                acc += jnp.dot(
                    xs[first : first + near // 2].reshape(tile, 3 * block),
                    taps[index, a].reshape(3 * block, outs),
                    preferred_element_type=f32,
                )
            for j in range(2):
                parts[index, j, side] = acc[:, j * block : (j + 1) * block].astype(bf16)
                target = 2 * col + j
                itself = jnp.logical_and(target == z, col == side)
                copy = remote(
                    parts.at[index, j, side],
                    sums.at[index, z],
                    rs_send.at[index, j, side],
                    rs_recv.at[index, z],
                    row=2 * target + x,
                    col=side,
                )

                @pl.when(itself)
                def _():
                    sums[index, z] = parts[index, j, side]

                @pl.when(jnp.logical_not(itself))
                def _():
                    copy.start()

    def partial_sent(index):
        for side in range(2):
            for j in range(2):
                target = 2 * col + j

                @pl.when(jnp.logical_not(jnp.logical_and(target == z, col == side)))
                def _():
                    remote(
                        parts.at[index, j, side],
                        sums.at[index, z],
                        rs_send.at[index, j, side],
                        rs_recv.at[index, z],
                        row=2 * target + x,
                        col=side,
                    ).wait_send()

    def reduced(index, bias):
        for origin in range(cuts):

            @pl.when(jnp.logical_not(jnp.logical_and(z == origin, z // 2 == col)))
            def _():
                remote(
                    parts.at[index, 0, 0],
                    sums.at[index, origin],
                    rs_send.at[index, 0, 0],
                    rs_recv.at[index, origin],
                    row=pair,
                ).wait_recv()

        result = sums[index, 0].astype(f32)
        for origin in range(1, cuts):
            result += sums[index, origin].astype(f32)
        return result + bias[:, here]

    partial_conv(0)
    start_taps(1)
    turn_ring(1)

    hidden = reduced(0, bias_one).astype(bf16)
    start = 1 + 2 * col
    hbuf[pl.ds(start, 2)] = hidden.reshape(2, width, block)
    hidden = hidden.astype(f32)
    group = 2 * x + col
    stats[group] = jnp.concatenate(
        [
            jnp.sum(hidden, axis=0, keepdims=True),
            jnp.sum(hidden * hidden, axis=0, keepdims=True),
            jnp.zeros((6, block), f32),
        ],
        axis=0,
    )
    for step, (target_row, target_col) in enumerate(((row, other), (pair, col), (pair, other))):
        copy = remote(
            stats.at[group],
            stats.at[group],
            h_send.at[step],
            h_recv.at[group],
            row=target_row,
            col=target_col,
        )
        copy.start()
        pending.append(copy)
    copy = remote(
        hbuf.at[pl.ds(start, 2)], hbuf.at[pl.ds(start, 2)], h_send.at[3], h_recv.at[4], col=other
    )
    copy.start()
    pending.append(copy)

    def edge(side):
        return remote(
            hbuf.at[near - (near - 1) * x],
            hbuf.at[(near + 1) * x],
            h_send.at[4 + side],
            h_recv.at[5],
            row=pair,
            col=side,
        )

    @pl.when(col == 1 - x)
    def _():
        for side in range(2):
            edge(side).start()

    turn_ring(2)
    for who in range(4):

        @pl.when(group != who)
        def _():
            remote(
                stats.at[who], stats.at[who], h_send.at[0], h_recv.at[who], row=pair
            ).wait_recv()

    theirs = hbuf.at[pl.ds(1 + 2 * other, 2)]
    remote(theirs, theirs, h_send.at[3], h_recv.at[4], col=other).wait_recv()
    remote(
        hbuf.at[0], hbuf.at[(near + 1) * (1 - x)], h_send.at[4], h_recv.at[5], row=pair
    ).wait_recv()
    both = stats[0] + stats[1] + stats[2] + stats[3]
    mean, factor = moments(both[0:1], both[1:2])
    for slot in range(near + 2):
        values = hbuf[slot].astype(f32)
        if slot == 0:
            values = jnp.where(x == 0, 0.0, values)
        if slot == near + 1:
            values = jnp.where(x == 1, 0.0, values)
        fill(slot, values, mean, factor, gain_two[:, here], shift_two[:, here])

    partial_conv(1)
    turn_ring(3)

    residual = jnp.concatenate(
        [feature_row(near * x + 2 * col), feature_row(near * x + 2 * col + 1)], axis=0
    )
    own_block[...] = (reduced(1, bias_two) + residual).astype(bf16).reshape(2, width, block)

    def block_copies(act):
        for k in range(2):
            origin = near * x + 2 * col + k
            for d in (-1, 0, 1):
                target = origin + d
                valid = jnp.logical_and(target >= 0, target < rows)
                itself = jnp.logical_and(target == row, z % 2 == col)
                act(k, d, target, valid, itself)

    def block_copy(k, d, target):
        return remote(
            own_block.at[k],
            b3.at[z % 2, 1 - d, z // 2],
            b_send.at[k, d + 1],
            b_recv.at[1 - d, z // 2],
            row=target,
            col=z % 2,
        )

    def begin(k, d, target, valid, itself):
        @pl.when(jnp.logical_and(valid, jnp.logical_not(itself)))
        def _():
            block_copy(k, d, target).start()

        @pl.when(itself)
        def _():
            b3[z % 2, 1 - d, z // 2] = own_block[k]

    def finish(k, d, target, valid, itself):
        @pl.when(jnp.logical_and(valid, jnp.logical_not(itself)))
        def _():
            block_copy(k, d, target).wait_send()

    block_copies(begin)
    turn_ring(4)
    for slot in range(3):
        source = row + slot - 1
        valid = jnp.logical_and(source >= 0, source < rows)
        for half in range(2):
            block_of = 2 * half + col
            itself = jnp.logical_and(
                jnp.logical_and(block_of == z, source // near == x), (source // 2) % 2 == col
            )

            @pl.when(jnp.logical_and(valid, jnp.logical_not(itself)))
            def _():
                remote(
                    own_block.at[0],
                    b3.at[col, slot, half],
                    b_send.at[0, 0],
                    b_recv.at[slot, half],
                    row=pair,
                ).wait_recv()

    copy = remote(b3.at[col], b3.at[col], b_send.at[2, 0], b_recv.at[3, 0], col=other)
    copy.start()
    pending.append(copy)
    remote(b3.at[other], b3.at[other], b_send.at[2, 0], b_recv.at[3, 0], col=other).wait_recv()

    for slot in range(3):
        for which in range(cuts):
            at = slice(which * block, (which + 1) * block)
            values = b3[which % 2, slot, which // 2]
            wide = values.astype(f32)
            x3[slot, 0, :, at] = jnp.where(first_column, 0.0, pltpu.roll(wide, 1, 0)).astype(bf16)
            x3[slot, 1, :, at] = values
            x3[slot, 2, :, at] = jnp.where(
                last_column, 0.0, pltpu.roll(wide, width - 1, 0)
            ).astype(bf16)

    local[2].wait()
    for way in range(2):
        for step in range(1, reach[way] + 1):
            cross_copy(way, step, 1 - img).wait_recv()

    acc = jnp.zeros((4 * width, outs), f32)
    for a in range(3):
        for c in range(3):
            window = jnp.concatenate(
                [
                    x3[(p + a - 1) // 2 + 1, (q + c - 1) // 2 + 1]
                    for p in range(2)
                    for q in range(2)
                ],
                axis=0,
            )
            acc += jnp.dot(window, gathered[a, c], preferred_element_type=f32)
    acc += bias_up[:, lanes]
    for p in range(2):
        for q in range(2):
            first = (2 * p + q) * width
            for lane in range(outs // 128):
                mixed[lane, p, pl.ds(q, width, stride=2), :] = acc[
                    first : first + width, lane * 128 : (lane + 1) * 128
                ]
    for p in range(2):
        for lane in range(outs // 128):
            at = slice(lane * 128, (lane + 1) * 128)
            swap[p, :, at] = mixed[
                lane, p, pl.ds(pl.multiple_of(other * width, width), width), :
            ].astype(bf16)
    copy = remote(swap, out.at[:, :, lanes], o_send.at[0], o_recv.at[0], col=other)
    copy.start()
    pending.append(copy)
    for p in range(2):
        for lane in range(outs // 128):
            at = pl.ds(pl.multiple_of(col * outs + lane * 128, 128), 128)
            out[p, :, at] = mixed[
                lane, p, pl.ds(pl.multiple_of(col * width, width), width), :
            ].astype(bf16)
    their_lanes = pl.ds(pl.multiple_of(other * outs, outs), outs)
    remote(swap, out.at[:, :, their_lanes], o_send.at[0], o_recv.at[0], col=other).wait_recv()

    for copy in pending:
        copy.wait_send()
    partial_sent(0)
    partial_sent(1)
    block_copies(finish)

    @pl.when(col == 1 - x)
    def _():
        for side in range(2):
            edge(side).wait_send()


def fused(
    features,
    first_gain,
    first_shift,
    first_weight,
    first_bias,
    second_gain,
    second_shift,
    second_weight,
    second_bias,
    upsample_weight,
    upsample_bias,
):
    _, half_width, channels = features.shape
    rows = lax.axis_size("row")
    cuts, near, width = rows // 2, rows // 2, 2 * half_width
    block, outs = channels // cuts, channels // 2
    bf16, f32 = jnp.bfloat16, jnp.float32
    dma = pltpu.SemaphoreType.DMA
    vmem = pl.BlockSpec(memory_space=pltpu.VMEM)
    anywhere = pl.BlockSpec(memory_space=pl.ANY)
    vectors = [
        v.reshape(1, channels)
        for v in (
            first_gain,
            first_shift,
            first_bias,
            second_gain,
            second_shift,
            second_bias,
            upsample_bias,
        )
    ]
    return pl.pallas_call(
        fused_kernel,
        out_shape=jax.ShapeDtypeStruct((2, width, channels), bf16),
        in_specs=[vmem] * 8 + [anywhere] * 3,
        out_specs=vmem,
        scratch_shapes=[
            pltpu.VMEM((2, rows, half_width, block), bf16),
            pltpu.VMEM((near + 2, width, 3 * block), bf16),
            pltpu.VMEM((2, 3, 3, block, outs), bf16),
            pltpu.VMEM((3, 3, channels, outs), bf16),
            pltpu.VMEM((2, 2, 2, near * width // 2, block), bf16),
            pltpu.VMEM((2, cuts, near * width // 2, block), bf16),
            pltpu.VMEM((near + 2, width, block), bf16),
            pltpu.VMEM((4, 8, block), f32),
            pltpu.VMEM((2, width, block), bf16),
            pltpu.VMEM((2, 3, 2, width, block), bf16),
            pltpu.VMEM((3, 3, width, channels), bf16),
            pltpu.VMEM((outs // 128, 2, 2 * width, 128), f32),
            pltpu.VMEM((2, width, outs), bf16),
            dma((3,)),
            dma((2,)),
            dma((2,)),
            dma((rows,)),
            dma((rows + 1,)),
            dma((2, 2, 2)),
            dma((2, cuts)),
            dma((6,)),
            dma((6,)),
            dma((3, 3)),
            dma((4, 2)),
            dma((2, near)),
            dma((2, near)),
            dma((2, near)),
            dma((2, near)),
            dma((1,)),
            dma((1,)),
        ],
        compiler_params=pltpu.CompilerParams(collective_id=0, has_side_effects=True),
    )(features.reshape(half_width, channels), *vectors, first_weight, second_weight, upsample_weight)


def program(features, *others):
    height, half_width, channels = features.shape
    rows = lax.axis_size("row")
    fits = (
        (lax.axis_size("img"), rows, lax.axis_size("col")) == (2, 8, 2)
        and height == 1
        and half_width % 16 == 0
        and channels == rows // 2 * 128
        and 128 % (channels // G) == 0
    )
    return (fused if fits else on_device)(features, *others)


def solution(mesh):
    return jax.shard_map(
        program,
        mesh=mesh,
        in_specs=(
            P(("img", "row"), "col", None),
            P(),
            P(),
            P(None, None, "row", None),
            P(),
            P(),
            P(),
            P(None, None, "row", None),
            P(),
            P(None, None, "row", None),
            P(),
        ),
        out_specs=P(("img", "row"), "col", None),
        check_vma=False,
    )
```

```python
import jax
import jax.numpy as jnp
from jax import lax
from jax.experimental import pallas as pl
from jax.experimental.pallas import tpu as pltpu
from jax.sharding import PartitionSpec as P

G = 32


EPS = 1e-06


def extended(cells, sides, width):
    for axis, dim in sides:
        count = lax.axis_size(axis)
        ends = count - 1
        head = lax.slice_in_dim(cells, 0, width, axis=dim)
        tail = lax.slice_in_dim(cells, cells.shape[dim] - width, cells.shape[dim], axis=dim)
        cells = jnp.concatenate(
            [
                lax.ppermute(tail, axis, [(i, (i + 1) % count) for i in range(ends)]),
                cells,
                lax.ppermute(head, axis, [((i + 1) % count, i) for i in range(ends)]),
            ],
            axis=dim,
        )
    return cells


def norm_silu(values, gain, shift):
    height, breadth, channels = values.shape
    grouped = values.reshape(height * breadth, G, channels // G)
    total = jnp.sum(grouped, axis=(0, 2))
    squares = jnp.sum(grouped * grouped, axis=(0, 2))
    total, squares = lax.psum((total, squares), ("row", "col"))
    count = height * breadth * lax.axis_size("row") * lax.axis_size("col") * (channels // G)
    mean = total / count
    var = squares / count - mean * mean
    factor = lax.rsqrt(var + EPS)
    normed = (grouped - mean[None, :, None]) * factor[None, :, None]
    normed = normed.reshape(height, breadth, channels) * gain + shift
    return jax.nn.silu(normed).astype(jnp.bfloat16)


def extend(values):
    return extended(values, (("row", 0), ("col", 1)), 1)


def convolve(padded, weight, bias, height, breadth):
    outputs = weight.shape[3]
    empty = jnp.zeros((height, breadth, outputs), jnp.float32)
    share = weight.shape[2] // lax.axis_size("col")
    own = lax.dynamic_slice_in_dim(weight, lax.axis_index("col") * share, share, 2)
    total = empty
    piece = lax.all_gather(own, ("row", "col"), axis=2, tiled=True)
    depth = piece.shape[2]
    offset = jnp.asarray(jnp.int32(0), jnp.int32)
    for offset_y in range(3):
        for offset_x in range(3):
            window = lax.dynamic_slice(
                padded, (jnp.int32(offset_y), jnp.int32(offset_x), offset), (height, breadth, depth)
            )
            total = total + jnp.einsum(
                "hwk,kc->hwc", window, piece[offset_y, offset_x], preferred_element_type=jnp.float32
            )
    return total + bias


def on_device(
    features,
    first_gain,
    first_shift,
    first_weight,
    first_bias,
    second_gain,
    second_shift,
    second_weight,
    second_bias,
    upsample_weight,
    upsample_bias,
):
    height, breadth, channels = features.shape
    normed_one = norm_silu(features.astype(jnp.float32), first_gain, first_shift)
    hidden = convolve(extend(normed_one), first_weight, first_bias, height, breadth).astype(
        jnp.bfloat16
    )
    normed_two = norm_silu(hidden.astype(jnp.float32), second_gain, second_shift)
    block_out = (
        convolve(extend(normed_two), second_weight, second_bias, height, breadth)
        + features.astype(jnp.float32)
    ).astype(jnp.bfloat16)
    doubled = jnp.repeat(jnp.repeat(block_out, 2, axis=0), 2, axis=1)
    padded = extend(doubled)
    return convolve(padded, upsample_weight, upsample_bias, 2 * height, 2 * breadth).astype(
        jnp.bfloat16
    )


def fused_kernel(
    features,
    gain_one,
    shift_one,
    bias_one,
    gain_two,
    shift_two,
    bias_two,
    bias_up,
    weight_one,
    weight_two,
    weight_up,
    out,
    fbuf,
    xs,
    taps,
    gathered,
    parts,
    sums,
    hbuf,
    stats,
    own_block,
    b3,
    x3,
    mixed,
    swap,
    local_sem,
    wx_send,
    wx_recv,
    f_send,
    f_recv,
    rs_send,
    rs_recv,
    h_send,
    h_recv,
    b_send,
    b_recv,
    ring_send,
    ring_recv,
    y_send,
    y_recv,
    o_send,
    o_recv,
):
    img = lax.axis_index("img")
    row = lax.axis_index("row")
    col = lax.axis_index("col")
    rows = lax.axis_size("row")
    cuts = rows // 2
    z, x = row // 2, row % 2
    other = 1 - col
    pair = row + 1 - 2 * x
    half_width, channels = features.shape
    width = 2 * half_width
    block = channels // cuts
    share = channels // rows
    outs = channels // 2
    near = rows // 2
    f32, bf16 = jnp.float32, jnp.bfloat16
    pending = []

    def remote(src, dst, send, recv, **device):
        return pltpu.make_async_remote_copy(
            src_ref=src,
            dst_ref=dst,
            send_sem=send,
            recv_sem=recv,
            device_id=device,
            device_id_type=pl.DeviceIdType.MESH,
        )

    zero_rows = jnp.zeros((2, width, block), bf16)
    for parity in range(2):
        for slot in (0, 2):
            b3[parity, slot] = zero_rows

    barrier = pltpu.get_barrier_semaphore()
    for step in range(rows):
        for side in range(2):
            if step or side:
                pl.semaphore_signal(
                    barrier,
                    inc=1,
                    device_id={"row": (row + step) % rows, "col": (col + side) % 2},
                    device_id_type=pl.DeviceIdType.MESH,
                )
    pl.semaphore_signal(
        barrier, inc=1, device_id={"img": 1 - img}, device_id_type=pl.DeviceIdType.MESH
    )
    lanes = pl.ds(pl.multiple_of(col * outs, outs), outs)
    mine = pl.ds(pl.multiple_of(x * share, share), share)
    local = []
    for index, weight in enumerate((weight_one, weight_two)):
        copy = pltpu.make_async_copy(
            weight.at[:, :, :, lanes], taps.at[index, :, :, mine, :], local_sem.at[index]
        )
        copy.start()
        local.append(copy)
    copy = pltpu.make_async_copy(
        weight_up.at[:, :, :, lanes],
        gathered.at[:, :, pl.ds(pl.multiple_of(row * share, share), share), :],
        local_sem.at[2],
    )
    copy.start()
    local.append(copy)
    pl.semaphore_wait(barrier, 2 * rows)

    def feature_copy(step):
        target = (row + step) % rows
        part = pl.ds(pl.multiple_of((target // 2) * block, block), block)
        return remote(
            features.at[:, part], fbuf.at[col, row], f_send.at[step], f_recv.at[row], row=target
        )

    for step in range(1, rows):
        copy = feature_copy(step)
        copy.start()
        pending.append(copy)
    fbuf[col, row] = features[:, pl.ds(pl.multiple_of(z * block, block), block)]

    def start_taps(index):
        copy = remote(
            (weight_one, weight_two)[index].at[:, :, :, lanes],
            taps.at[index, :, :, mine, :],
            wx_send.at[index],
            wx_recv.at[index],
            row=pair,
        )
        copy.start()
        pending.append(copy)

    for index, weight in enumerate((weight_one, weight_two)):
        if index == 0:
            start_taps(0)
    place = z * (1 - x) + (rows - 1 - z) * x
    piece = share // 2

    def row_at(position):
        side = position // near
        return (1 - side) * 2 * position + side * (2 * (rows - 1 - position) + 1)

    after = row_at((place + 1) % rows)
    before = row_at((place + rows - 1) % rows)

    def unit(position, part):
        return gathered.at[
            :, :, pl.ds(pl.multiple_of(row_at(position) * share + part * piece, piece), piece), :
        ]

    def ring_copy(way, step):
        position = (place + rows - (step - 1)) % rows if way == 0 else (place + step - 1) % rows
        if step == 1:
            src = weight_up.at[:, :, pl.ds(pl.multiple_of(img * piece, piece), piece), lanes]
        else:
            src = unit(position, img)
        return remote(
            src,
            unit(position, img),
            ring_send.at[way, step - 1],
            ring_recv.at[way, step - 1],
            row=after if way == 0 else before,
        )

    reach = (near, rows - 1 - near)

    def cross_copy(way, step, half):
        position = (place + rows - step) % rows if way == 0 else (place + step) % rows
        return remote(
            unit(position, half),
            unit(position, half),
            y_send.at[way, step - 1],
            y_recv.at[way, step - 1],
            img=1 - img,
        )

    def start_ring(step):
        for way in range(2):
            if step <= reach[way]:
                copy = ring_copy(way, step)
                copy.start()
                pending.append(copy)

    def arrived_ring(way, step):
        position = (place + rows - step) % rows if way == 0 else (place + step) % rows
        return remote(
            unit(position, img),
            unit(position, img),
            ring_send.at[way, step - 1],
            ring_recv.at[way, step - 1],
            row=after,
        )

    def turn_ring(step):
        for way in range(2):
            if step <= reach[way]:
                arrived_ring(way, step).wait_recv()
        start_ring(step + 1)
        for way in range(2):
            if step <= reach[way]:
                copy = cross_copy(way, step, img)
                copy.start()
                pending.append(copy)

    start_ring(1)

    for step in range(1, rows):
        origin = (row + step) % rows
        remote(
            features.at[:, pl.ds(0, block)],
            fbuf.at[col, origin],
            f_send.at[step],
            f_recv.at[origin],
            row=pair,
        ).wait_recv()
    copy = remote(fbuf.at[col], fbuf.at[col], f_send.at[0], f_recv.at[rows], col=other)
    copy.start()
    pending.append(copy)
    remote(fbuf.at[other], fbuf.at[other], f_send.at[0], f_recv.at[rows], col=other).wait_recv()

    same = (
        lax.broadcasted_iota(jnp.int32, (block, block), 0) // (channels // G)
        == lax.broadcasted_iota(jnp.int32, (block, block), 1) // (channels // G)
    ).astype(f32)
    count = rows * width * (channels // G)

    def moments(total, squares):
        both = jnp.concatenate([total, squares, jnp.zeros((6, block), f32)], axis=0)
        both = jnp.dot(both, same, precision=lax.Precision.HIGHEST, preferred_element_type=f32)
        mean = both[0:1] / count
        var = both[1:2] / count - mean * mean
        return mean, lax.rsqrt(var + EPS)

    here = pl.ds(pl.multiple_of(z * block, block), block)
    first_column = lax.broadcasted_iota(jnp.int32, (width, block), 0) == 0
    last_column = lax.broadcasted_iota(jnp.int32, (width, block), 0) == width - 1

    def fill(slot, values, mean, factor, gain, shift):
        normed = (values - mean) * factor * gain + shift
        normed = normed / (1.0 + jnp.exp(-normed))
        if slot == 0:
            normed = jnp.where(x == 0, 0.0, normed)
        if slot == near + 1:
            normed = jnp.where(x == 1, 0.0, normed)
        left = jnp.where(first_column, 0.0, pltpu.roll(normed, 1, 0))
        right = jnp.where(last_column, 0.0, pltpu.roll(normed, width - 1, 0))
        xs[slot, :, 0:block] = left.astype(bf16)
        xs[slot, :, block : 2 * block] = normed.astype(bf16)
        xs[slot, :, 2 * block : 3 * block] = right.astype(bf16)

    def feature_row(index):
        return jnp.concatenate([fbuf[0, index], fbuf[1, index]], axis=0).astype(f32)

    total = jnp.zeros((1, block), f32)
    squares = jnp.zeros((1, block), f32)
    for index in range(rows):
        values = feature_row(index)
        total += jnp.sum(values, axis=0, keepdims=True)
        squares += jnp.sum(values * values, axis=0, keepdims=True)
    mean, factor = moments(total, squares)
    for slot in range(near + 2):
        index = jnp.clip(near * x - 1 + slot, 0, rows - 1)
        fill(slot, feature_row(index), mean, factor, gain_one[:, here], shift_one[:, here])

    tile = near * width // 2

    def partial_conv(index):
        local[index].wait()
        remote(
            weight_one.at[:, :, :, lanes],
            taps.at[index, :, :, pl.ds(pl.multiple_of((1 - x) * share, share), share), :],
            wx_send.at[index],
            wx_recv.at[index],
            row=pair,
        ).wait_recv()
        for side in range(2):
            acc = jnp.zeros((tile, outs), f32)
            for a in range(3):
                first = a + side * near // 2
                acc += jnp.dot(
                    xs[first : first + near // 2].reshape(tile, 3 * block),
                    taps[index, a].reshape(3 * block, outs),
                    preferred_element_type=f32,
                )
            for j in range(2):
                parts[index, j, side] = acc[:, j * block : (j + 1) * block].astype(bf16)
                target = 2 * col + j
                itself = jnp.logical_and(target == z, col == side)
                copy = remote(
                    parts.at[index, j, side],
                    sums.at[index, z],
                    rs_send.at[index, j, side],
                    rs_recv.at[index, z],
                    row=2 * target + x,
                    col=side,
                )

                @pl.when(itself)
                def _():
                    sums[index, z] = parts[index, j, side]

                @pl.when(jnp.logical_not(itself))
                def _():
                    copy.start()

    def partial_sent(index):
        for side in range(2):
            for j in range(2):
                target = 2 * col + j

                @pl.when(jnp.logical_not(jnp.logical_and(target == z, col == side)))
                def _():
                    remote(
                        parts.at[index, j, side],
                        sums.at[index, z],
                        rs_send.at[index, j, side],
                        rs_recv.at[index, z],
                        row=2 * target + x,
                        col=side,
                    ).wait_send()

    def reduced(index, bias):
        for origin in range(cuts):

            @pl.when(jnp.logical_not(jnp.logical_and(z == origin, z // 2 == col)))
            def _():
                remote(
                    parts.at[index, 0, 0],
                    sums.at[index, origin],
                    rs_send.at[index, 0, 0],
                    rs_recv.at[index, origin],
                    row=pair,
                ).wait_recv()

        result = sums[index, 0].astype(f32)
        for origin in range(1, cuts):
            result += sums[index, origin].astype(f32)
        return result + bias[:, here]

    partial_conv(0)
    start_taps(1)
    turn_ring(1)

    hidden = reduced(0, bias_one).astype(bf16)
    start = 1 + 2 * col
    hbuf[pl.ds(start, 2)] = hidden.reshape(2, width, block)
    hidden = hidden.astype(f32)
    group = 2 * x + col
    stats[group] = jnp.concatenate(
        [
            jnp.sum(hidden, axis=0, keepdims=True),
            jnp.sum(hidden * hidden, axis=0, keepdims=True),
            jnp.zeros((6, block), f32),
        ],
        axis=0,
    )
    for step, (target_row, target_col) in enumerate(((row, other), (pair, col), (pair, other))):
        copy = remote(
            stats.at[group],
            stats.at[group],
            h_send.at[step],
            h_recv.at[group],
            row=target_row,
            col=target_col,
        )
        copy.start()
        pending.append(copy)
    copy = remote(
        hbuf.at[pl.ds(start, 2)], hbuf.at[pl.ds(start, 2)], h_send.at[3], h_recv.at[4], col=other
    )
    copy.start()
    pending.append(copy)

    def edge(side):
        return remote(
            hbuf.at[near - (near - 1) * x],
            hbuf.at[(near + 1) * x],
            h_send.at[4 + side],
            h_recv.at[5],
            row=pair,
            col=side,
        )

    @pl.when(col == 1 - x)
    def _():
        for side in range(2):
            edge(side).start()

    turn_ring(2)
    for who in range(4):

        @pl.when(group != who)
        def _():
            remote(
                stats.at[who], stats.at[who], h_send.at[0], h_recv.at[who], row=pair
            ).wait_recv()

    theirs = hbuf.at[pl.ds(1 + 2 * other, 2)]
    remote(theirs, theirs, h_send.at[3], h_recv.at[4], col=other).wait_recv()
    remote(
        hbuf.at[0], hbuf.at[(near + 1) * (1 - x)], h_send.at[4], h_recv.at[5], row=pair
    ).wait_recv()
    both = stats[0] + stats[1] + stats[2] + stats[3]
    mean, factor = moments(both[0:1], both[1:2])
    for slot in range(near + 2):
        values = hbuf[slot].astype(f32)
        if slot == 0:
            values = jnp.where(x == 0, 0.0, values)
        if slot == near + 1:
            values = jnp.where(x == 1, 0.0, values)
        fill(slot, values, mean, factor, gain_two[:, here], shift_two[:, here])

    partial_conv(1)
    turn_ring(3)

    residual = jnp.concatenate(
        [feature_row(near * x + 2 * col), feature_row(near * x + 2 * col + 1)], axis=0
    )
    own_block[...] = (reduced(1, bias_two) + residual).astype(bf16).reshape(2, width, block)

    def block_copies(act):
        for k in range(2):
            origin = near * x + 2 * col + k
            for d in (-1, 0, 1):
                target = origin + d
                valid = jnp.logical_and(target >= 0, target < rows)
                itself = jnp.logical_and(target == row, z % 2 == col)
                act(k, d, target, valid, itself)

    def block_copy(k, d, target):
        return remote(
            own_block.at[k],
            b3.at[z % 2, 1 - d, z // 2],
            b_send.at[k, d + 1],
            b_recv.at[1 - d, z // 2],
            row=target,
            col=z % 2,
        )

    def begin(k, d, target, valid, itself):
        @pl.when(jnp.logical_and(valid, jnp.logical_not(itself)))
        def _():
            block_copy(k, d, target).start()

        @pl.when(itself)
        def _():
            b3[z % 2, 1 - d, z // 2] = own_block[k]

    def finish(k, d, target, valid, itself):
        @pl.when(jnp.logical_and(valid, jnp.logical_not(itself)))
        def _():
            block_copy(k, d, target).wait_send()

    block_copies(begin)
    turn_ring(4)
    for slot in range(3):
        source = row + slot - 1
        valid = jnp.logical_and(source >= 0, source < rows)
        for half in range(2):
            block_of = 2 * half + col
            itself = jnp.logical_and(
                jnp.logical_and(block_of == z, source // near == x), (source // 2) % 2 == col
            )

            @pl.when(jnp.logical_and(valid, jnp.logical_not(itself)))
            def _():
                remote(
                    own_block.at[0],
                    b3.at[col, slot, half],
                    b_send.at[0, 0],
                    b_recv.at[slot, half],
                    row=pair,
                ).wait_recv()

    copy = remote(b3.at[col], b3.at[col], b_send.at[2, 0], b_recv.at[3, 0], col=other)
    copy.start()
    pending.append(copy)
    remote(b3.at[other], b3.at[other], b_send.at[2, 0], b_recv.at[3, 0], col=other).wait_recv()

    for slot in range(3):
        for which in range(cuts):
            at = slice(which * block, (which + 1) * block)
            values = b3[which % 2, slot, which // 2]
            wide = values.astype(f32)
            x3[slot, 0, :, at] = jnp.where(first_column, 0.0, pltpu.roll(wide, 1, 0)).astype(bf16)
            x3[slot, 1, :, at] = values
            x3[slot, 2, :, at] = jnp.where(
                last_column, 0.0, pltpu.roll(wide, width - 1, 0)
            ).astype(bf16)

    local[2].wait()
    for way in range(2):
        for step in range(1, reach[way] + 1):
            cross_copy(way, step, 1 - img).wait_recv()

    acc = jnp.zeros((4 * width, outs), f32)
    for a in range(3):
        for c in range(3):
            window = jnp.concatenate(
                [
                    x3[(p + a - 1) // 2 + 1, (q + c - 1) // 2 + 1]
                    for p in range(2)
                    for q in range(2)
                ],
                axis=0,
            )
            acc += jnp.dot(window, gathered[a, c], preferred_element_type=f32)
    acc += bias_up[:, lanes]
    for p in range(2):
        for q in range(2):
            first = (2 * p + q) * width
            for lane in range(outs // 128):
                mixed[lane, p, pl.ds(q, width, stride=2), :] = acc[
                    first : first + width, lane * 128 : (lane + 1) * 128
                ]
    for p in range(2):
        for lane in range(outs // 128):
            at = slice(lane * 128, (lane + 1) * 128)
            swap[p, :, at] = mixed[
                lane, p, pl.ds(pl.multiple_of(other * width, width), width), :
            ].astype(bf16)
    copy = remote(swap, out.at[:, :, lanes], o_send.at[0], o_recv.at[0], col=other)
    copy.start()
    pending.append(copy)
    for p in range(2):
        for lane in range(outs // 128):
            at = pl.ds(pl.multiple_of(col * outs + lane * 128, 128), 128)
            out[p, :, at] = mixed[
                lane, p, pl.ds(pl.multiple_of(col * width, width), width), :
            ].astype(bf16)
    their_lanes = pl.ds(pl.multiple_of(other * outs, outs), outs)
    remote(swap, out.at[:, :, their_lanes], o_send.at[0], o_recv.at[0], col=other).wait_recv()

    for copy in pending:
        copy.wait_send()
    partial_sent(0)
    partial_sent(1)
    block_copies(finish)

    @pl.when(col == 1 - x)
    def _():
        for side in range(2):
            edge(side).wait_send()


def fused(
    features,
    first_gain,
    first_shift,
    first_weight,
    first_bias,
    second_gain,
    second_shift,
    second_weight,
    second_bias,
    upsample_weight,
    upsample_bias,
):
    _, half_width, channels = features.shape
    rows = lax.axis_size("row")
    cuts, near, width = rows // 2, rows // 2, 2 * half_width
    block, outs = channels // cuts, channels // 2
    bf16, f32 = jnp.bfloat16, jnp.float32
    dma = pltpu.SemaphoreType.DMA
    vmem = pl.BlockSpec(memory_space=pltpu.VMEM)
    anywhere = pl.BlockSpec(memory_space=pl.ANY)
    vectors = [
        v.reshape(1, channels)
        for v in (
            first_gain,
            first_shift,
            first_bias,
            second_gain,
            second_shift,
            second_bias,
            upsample_bias,
        )
    ]
    return pl.pallas_call(
        fused_kernel,
        out_shape=jax.ShapeDtypeStruct((2, width, channels), bf16),
        in_specs=[vmem] * 8 + [anywhere] * 3,
        out_specs=vmem,
        scratch_shapes=[
            pltpu.VMEM((2, rows, half_width, block), bf16),
            pltpu.VMEM((near + 2, width, 3 * block), bf16),
            pltpu.VMEM((2, 3, 3, block, outs), bf16),
            pltpu.VMEM((3, 3, channels, outs), bf16),
            pltpu.VMEM((2, 2, 2, near * width // 2, block), bf16),
            pltpu.VMEM((2, cuts, near * width // 2, block), bf16),
            pltpu.VMEM((near + 2, width, block), bf16),
            pltpu.VMEM((4, 8, block), f32),
            pltpu.VMEM((2, width, block), bf16),
            pltpu.VMEM((2, 3, 2, width, block), bf16),
            pltpu.VMEM((3, 3, width, channels), bf16),
            pltpu.VMEM((outs // 128, 2, 2 * width, 128), f32),
            pltpu.VMEM((2, width, outs), bf16),
            dma((3,)),
            dma((2,)),
            dma((2,)),
            dma((rows,)),
            dma((rows + 1,)),
            dma((2, 2, 2)),
            dma((2, cuts)),
            dma((6,)),
            dma((6,)),
            dma((3, 3)),
            dma((4, 2)),
            dma((2, near)),
            dma((2, near)),
            dma((2, near)),
            dma((2, near)),
            dma((1,)),
            dma((1,)),
        ],
        compiler_params=pltpu.CompilerParams(collective_id=0, has_side_effects=True),
    )(features.reshape(half_width, channels), *vectors, first_weight, second_weight, upsample_weight)


def program(features, *others):
    height, half_width, channels = features.shape
    rows = lax.axis_size("row")
    fits = (
        (lax.axis_size("img"), rows, lax.axis_size("col")) == (2, 8, 2)
        and height == 1
        and half_width % 16 == 0
        and channels == rows // 2 * 128
        and 128 % (channels // G) == 0
    )
    return (fused if fits else on_device)(features, *others)


def solution(mesh):
    return jax.shard_map(
        program,
        mesh=mesh,
        in_specs=(
            P(("img", "row"), "col", None),
            P(),
            P(),
            P(None, None, "row", None),
            P(),
            P(),
            P(),
            P(None, None, "row", None),
            P(),
            P(None, None, "row", None),
            P(),
        ),
        out_specs=P(("img", "row"), "col", None),
        check_vma=False,
    )
```
